32 devices in a mesh: wide: 8 (over z, x), narrow: 4 (over y, core).
Axes of the slice: x: 2, y: 2, z: 4, core: 2. Of those that a mesh axis runs over, the one named last changes fastest.
Arguments:
- cost: float32 [1024, 16384], P('wide', 'narrow'), may hold values from 0 to 2
- plan: float32 [1024, 16384], P('wide', 'narrow'), may hold values from 0 to 2
- row_mass: float32 [1024], P('wide'), may hold values from 4096 to 28672
- col_mass: float32 [16384], P('narrow'), may hold values from 256 to 1792
- row_dual: float32 [1024], P('wide'), may hold values from -3 to 3
- col_dual: float32 [16384], P('narrow'), may hold values from -3 to 3
Outputs:
- plan_out: float32 [1024, 16384], P('wide', 'narrow')
- row_out: float32 [1024], P('wide')
- col_out: float32 [16384], P('narrow')
The draws below stay inside these ranges and needn't reach their ends.
All inputs are finite; a program needn't handle non-finite values.
Results may differ from the reference program's by a relative error of at most 0.0001.
Values sent between devices are 32-bit elements; how exact they have to be, the bound alone decides.
A program may use at most 64 MiB of HBM per device.

```python
import math
import jax
import jax.numpy as jnp
from jax import lax

ITERS = 4
NR = 1024
NC = 16384


def block_scale(rng, extent, shards, smallest, largest):
    level, own = 1.0, jax.random.fold_in(rng, 6)
    for position, parts in shards:
        heights = jnp.exp(jax.random.uniform(jax.random.fold_in(own, position), (parts,), jnp.float32, smallest / len(shards), largest / len(shards)))
        level = level * jnp.repeat(heights, extent[position] // parts).reshape([-1 if axis == position else 1 for axis in range(len(extent))])
    return level


def bell_draw(rng, extent, width, limit, split=(), dtype=jnp.bfloat16):
    gain = block_scale(rng, extent, split, -0.22, 0.18) if split else 1.0
    entries = jax.random.normal(rng, extent, jnp.float32) * width * gain
    return jnp.minimum(jnp.maximum(entries, -limit), limit).astype(dtype)


def setup_inputs(seed: int = 0) -> dict:
    keys = jax.random.split(jax.random.key(seed), 7)
    cost = jnp.clip(2.0 * jax.random.uniform(keys[0], (NR, NC), jnp.float32) ** block_scale(keys[0], (NR, NC), ((0, 8), (1, 4)), -0.2, 0.2), 0.0, 2.0)
    plan = jnp.clip(2.0 * jax.random.uniform(keys[1], (NR, NC), jnp.float32) ** block_scale(keys[1], (NR, NC), ((0, 8), (1, 4)), -0.2, 0.2), 0.0, 2.0)
    row_mass = jnp.clip(4096.0 + 24576.0 * jax.random.uniform(keys[2], (NR,), jnp.float32) ** block_scale(keys[2], (NR,), ((0, 8),), -0.2, 0.2), 4096.0, 28672.0)
    col_mass = jnp.clip(256.0 + 1536.0 * jax.random.uniform(keys[3], (NC,), jnp.float32) ** block_scale(keys[3], (NC,), ((0, 4),), -0.2, 0.2), 256.0, 1792.0)
    row_dual = bell_draw(keys[4], (NR,), 0.5, 3.0, ((0, 8),), jnp.float32)
    col_dual = bell_draw(keys[5], (NC,), 0.5, 3.0, ((0, 4),), jnp.float32)
    return dict(cost=cost, plan=plan, row_mass=row_mass, col_mass=col_mass, row_dual=row_dual, col_dual=col_dual)


def reference(cost, plan, row_mass, col_mass, row_dual, col_dual):
    step_base = 0.9 / math.sqrt(NR + NC)
    weight = jnp.float32(step_base)
    for step in range(ITERS):
        primal_step = step_base / weight
        dual_step = step_base * weight
        fresh = jnp.maximum(plan - primal_step * (cost - row_dual[:, None] - col_dual[None, :]), 0.0)
        change = fresh - plan
        extrap = fresh + change
        moved = jnp.sum(change * change)
        new_row = row_dual + dual_step * (row_mass - lax.optimization_barrier(jnp.sum(extrap, axis=1)))
        new_col = col_dual + dual_step * (col_mass - lax.optimization_barrier(jnp.sum(extrap, axis=0)))
        dual_moved = jnp.sum((new_row - row_dual) ** 2) + jnp.sum((new_col - col_dual) ** 2)
        weight = jnp.sqrt(weight * jnp.sqrt((dual_moved + 1.0) / (moved + 1.0)))
        plan, row_dual, col_dual = (fresh, new_row, new_col)
    return (plan, row_dual, col_dual)
```

```python
import functools
import math

import jax
import jax.numpy as jnp
from jax import lax
from jax.experimental import pallas as pl
from jax.experimental.pallas import tpu as pltpu
from jax.sharding import PartitionSpec as P

ITERS = 4
LANES = 128
BLOCKS = 8
MESH = pl.DeviceIdType.MESH


def kernel(
    W, N, G, step_base,
    cost_hbm, plan_hbm, rmass_ref, cmass_ref, u_ref, v_ref,
    plan_out, u_out, v_out,
    cost, plan, colbuf, ub, ucur, V, SB, RB, RP, RH, SC,
    in_sem, out_sem,
    s1_send, s1_recv, row_send, row_recv, rho_send, rho_recv,
    v_send, v_recv, sc_send, sc_recv,
):
    rows, cols = plan.shape
    chunks = cols // LANES
    part = chunks // G
    per_block = chunks // BLOCKS
    width = per_block * LANES
    w = lax.axis_index("wide")
    n = lax.axis_index("narrow")
    h = lax.rem(w, G)
    base = w - h

    loads = []
    for b in range(BLOCKS):
        sl = (slice(None), pl.ds(b * width, width))
        pair = (
            pltpu.make_async_copy(cost_hbm.at[sl], cost.at[sl], in_sem.at[0, b]),
            pltpu.make_async_copy(plan_hbm.at[sl], plan.at[sl], in_sem.at[1, b]),
        )
        for copy in pair:
            copy.start()
        loads.append(pair)

    wide_peers = [(lax.rem(w + d, W), lax.rem(w + W - d, W)) for d in range(1, W)]
    narrow_peers = [(lax.rem(n + d, N), lax.rem(n + N - d, N)) for d in range(1, N)]
    block_peers = []
    for dh in range(G):
        for dn in range(N):
            if dh == 0 and dn == 0:
                continue
            hp, hs = lax.rem(h + dh, G), lax.rem(h + G - dh, G)
            np_, ns = lax.rem(n + dn, N), lax.rem(n + N - dn, N)
            block_peers.append((dh, dn, hp, np_, hs, ns))

    barrier = pltpu.get_barrier_semaphore()
    greeted = 0
    for to, _ in wide_peers:
        pl.semaphore_signal(barrier, inc=1, device_id=(to, n), device_id_type=MESH)
        greeted += 1
    for to, _ in narrow_peers:
        pl.semaphore_signal(barrier, inc=1, device_id=(w, to), device_id_type=MESH)
        greeted += 1
    for dh, dn, hp, np_, _, _ in block_peers:
        if dh and dn:
            pl.semaphore_signal(barrier, inc=1, device_id=(base + hp, np_), device_id_type=MESH)
            greeted += 1

    def spread(row):
        return jnp.broadcast_to(row, (LANES, LANES)).T

    def to_lanes(acc):
        return jnp.concatenate(
            [
                jnp.sum(acc[g * LANES:(g + 1) * LANES].T, axis=0, keepdims=True)
                for g in range(rows // LANES)
            ],
            axis=0,
        )

    for g in range(rows // LANES):
        ub[g * LANES:(g + 1) * LANES, :] = spread(u_ref[g:g + 1, :])
    ucur[...] = u_ref[...]
    for g in range(G):
        V[0, g] = v_ref[g * part:(g + 1) * part, :]

    weight = jnp.full((1, 1), step_base, jnp.float32)
    pending = []
    stores = []
    for k in range(ITERS):
        last = k == ITERS - 1
        primal = step_base / weight
        dual = step_base * weight
        tau = jnp.broadcast_to(primal, (1, LANES))

        def chunk(c, carry, k=k, tau=tau):
            racc, macc = carry
            lanes = pl.ds(pl.multiple_of(c * LANES, LANES), LANES)
            x = plan[:, lanes]
            g, r = c // part, c % part
            v = V[k, g, pl.ds(r, 1), :]
            f = jnp.maximum(x - tau * (cost[:, lanes] - ub[...] - v), 0.0)
            ch = f - x
            plan[:, lanes] = f
            ext = f + ch
            colbuf[pl.ds(c, 1), :] = jnp.sum(ext, axis=0, keepdims=True)
            sq = ch * ch
            return racc + ext, macc + jnp.sum(sq.reshape(rows // 8, 8, LANES), axis=0)

        carry = (jnp.zeros((rows, LANES), jnp.float32), jnp.zeros((8, LANES), jnp.float32))
        if k == 0:
            for b in range(BLOCKS):
                for copy in loads[b]:
                    copy.wait()
                carry = lax.fori_loop(b * per_block, (b + 1) * per_block, chunk, carry, unroll=2)
        elif last:
            for b in range(BLOCKS):
                carry = lax.fori_loop(b * per_block, (b + 1) * per_block, chunk, carry, unroll=2)
                sl = (slice(None), pl.ds(b * width, width))
                copy = pltpu.make_async_copy(plan.at[sl], plan_out.at[sl], out_sem.at[b])
                copy.start()
                stores.append(copy)
        else:
            carry = lax.fori_loop(0, chunks, chunk, carry, unroll=2)
        racc, macc = carry

        moved_row = jnp.sum(macc, axis=0, keepdims=True)
        for g in range(G):
            SB[k, g, 0:part, :] = colbuf[g * part:(g + 1) * part, :]
            SB[k, g, part:part + 1, :] = moved_row
        if k == 0:
            pl.semaphore_wait(barrier, greeted)
        waits1 = []
        for d, (to, src) in enumerate(wide_peers):
            copy = pltpu.make_async_remote_copy(
                src_ref=SB.at[k, lax.rem(to, G)], dst_ref=RB.at[k, w],
                send_sem=s1_send.at[k, d], recv_sem=s1_recv.at[k, w],
                device_id=(to, n), device_id_type=MESH)
            copy.start()
            pending.append(copy)
            waits1.append(pltpu.make_async_remote_copy(
                src_ref=SB.at[k, 0], dst_ref=RB.at[k, src],
                send_sem=s1_send.at[k, d], recv_sem=s1_recv.at[k, src],
                device_id=(to, n), device_id_type=MESH))
        RP[k, n] = to_lanes(racc)
        waits = []
        for d, (to, src) in enumerate(narrow_peers):
            copy = pltpu.make_async_remote_copy(
                src_ref=RP.at[k, n], dst_ref=RP.at[k, n],
                send_sem=row_send.at[k, d], recv_sem=row_recv.at[k, n],
                device_id=(w, to), device_id_type=MESH)
            copy.start()
            pending.append(copy)
            waits.append(pltpu.make_async_remote_copy(
                src_ref=RP.at[k, src], dst_ref=RP.at[k, src],
                send_sem=row_send.at[k, d], recv_sem=row_recv.at[k, src],
                device_id=(w, to), device_id_type=MESH))
        RB[k, w] = SB[k, h]
        for copy in waits:
            copy.wait_recv()
        total = RP[k, 0]
        for i in range(1, N):
            total = total + RP[k, i]
        u_old = ucur[...]
        u_new = u_old + dual * (rmass_ref[...] - total)
        if last:
            u_out[...] = u_new
        else:
            rho = jnp.sum((u_new - u_old) ** 2, axis=0, keepdims=True)
            RH[k, w] = rho
            waits_rho = []
            for d, (to, src) in enumerate(wide_peers):
                copy = pltpu.make_async_remote_copy(
                    src_ref=RH.at[k, w], dst_ref=RH.at[k, w],
                    send_sem=rho_send.at[k, d], recv_sem=rho_recv.at[k, w],
                    device_id=(to, n), device_id_type=MESH)
                copy.start()
                pending.append(copy)
                waits_rho.append(pltpu.make_async_remote_copy(
                    src_ref=RH.at[k, src], dst_ref=RH.at[k, src],
                    send_sem=rho_send.at[k, d], recv_sem=rho_recv.at[k, src],
                    device_id=(to, n), device_id_type=MESH))
            ucur[...] = u_new
            for g in range(rows // LANES):
                ub[g * LANES:(g + 1) * LANES, :] = spread(u_new[g:g + 1, :])

        for copy in waits1:
            copy.wait_recv()
        both = RB[k, 0]
        for i in range(1, W):
            both = both + RB[k, i]
        v_old = V[k, h]
        mass = cmass_ref[pl.ds(pl.multiple_of(h * part, part), part), :]
        v_new = v_old + dual * (mass - both[0:part])
        V[k + 1, h] = v_new
        v_waits = []
        sc_waits = []
        if not last:
            mine = h * N + n
            SC[k, mine, 0:1, :] = jnp.sum((v_new - v_old) ** 2, axis=0, keepdims=True)
            SC[k, mine, 1:2, :] = both[part:part + 1]
        for i, (dh, dn, hp, np_, hs, ns) in enumerate(block_peers):
            if dh and dn == 0:
                copy = pltpu.make_async_remote_copy(
                    src_ref=V.at[k + 1, h], dst_ref=V.at[k + 1, h],
                    send_sem=v_send.at[k, dh], recv_sem=v_recv.at[k, h],
                    device_id=(base + hp, n), device_id_type=MESH)
                copy.start()
                pending.append(copy)
                v_waits.append(pltpu.make_async_remote_copy(
                    src_ref=V.at[k + 1, hs], dst_ref=V.at[k + 1, hs],
                    send_sem=v_send.at[k, dh], recv_sem=v_recv.at[k, hs],
                    device_id=(base + hp, n), device_id_type=MESH))
            if not last:
                theirs = hs * N + ns
                copy = pltpu.make_async_remote_copy(
                    src_ref=SC.at[k, mine], dst_ref=SC.at[k, mine],
                    send_sem=sc_send.at[k, i], recv_sem=sc_recv.at[k, mine],
                    device_id=(base + hp, np_), device_id_type=MESH)
                copy.start()
                pending.append(copy)
                sc_waits.append(pltpu.make_async_remote_copy(
                    src_ref=SC.at[k, theirs], dst_ref=SC.at[k, theirs],
                    send_sem=sc_send.at[k, i], recv_sem=sc_recv.at[k, theirs],
                    device_id=(base + hp, np_), device_id_type=MESH))
        if not last:
            for copy in waits_rho:
                copy.wait_recv()
            squares = RH[k, 0]
            for i in range(1, W):
                squares = squares + RH[k, i]
            for copy in sc_waits:
                copy.wait_recv()
            for i in range(G * N):
                squares = squares + SC[k, i, 0:1, :]
            moved = SC[k, 0, 1:2, :]
            for i in range(1, N):
                moved = moved + SC[k, i, 1:2, :]
            dual_moved = jnp.sum(squares, axis=1, keepdims=True)
            moved = jnp.sum(moved, axis=1, keepdims=True)
            weight = jnp.sqrt(weight * jnp.sqrt((dual_moved + 1.0) / (moved + 1.0)))
        for copy in v_waits:
            copy.wait_recv()
    for g in range(G):
        v_out[g * part:(g + 1) * part, :] = V[ITERS, g]
    for copy in pending:
        copy.wait_send()
    for copy in stores:
        copy.wait()


def shards(W, N, G, cost, plan, row_mass, col_mass, row_dual, col_dual):
    rows, cols = plan.shape
    step_base = 0.9 / math.sqrt(rows * W + cols * N)
    chunks = cols // LANES
    part = chunks // G
    groups = rows // LANES
    f32 = jnp.float32
    dma = pltpu.SemaphoreType.DMA
    vmem = pl.BlockSpec(memory_space=pltpu.VMEM)
    hbm = pl.BlockSpec(memory_space=pl.ANY)
    plan_out, u_out, v_out = pl.pallas_call(
        functools.partial(kernel, W, N, G, step_base),
        out_shape=(
            jax.ShapeDtypeStruct((rows, cols), f32),
            jax.ShapeDtypeStruct((groups, LANES), f32),
            jax.ShapeDtypeStruct((chunks, LANES), f32),
        ),
        in_specs=[hbm, hbm, vmem, vmem, vmem, vmem],
        out_specs=(hbm, vmem, vmem),
        scratch_shapes=[
            pltpu.VMEM((rows, cols), f32),
            pltpu.VMEM((rows, cols), f32),
            pltpu.VMEM((chunks, LANES), f32),
            pltpu.VMEM((rows, LANES), f32),
            pltpu.VMEM((groups, LANES), f32),
            pltpu.VMEM((ITERS + 1, G, part, LANES), f32),
            pltpu.VMEM((ITERS, G, part + 1, LANES), f32),
            pltpu.VMEM((ITERS, W, part + 1, LANES), f32),
            pltpu.VMEM((ITERS, N, groups, LANES), f32),
            pltpu.VMEM((ITERS, W, 1, LANES), f32),
            pltpu.VMEM((ITERS, G * N, 2, LANES), f32),
            dma((2, BLOCKS)), dma((BLOCKS,)),
            dma((ITERS, W)), dma((ITERS, W)),
            dma((ITERS, N)), dma((ITERS, N)),
            dma((ITERS, W)), dma((ITERS, W)),
            dma((ITERS, G)), dma((ITERS, G)),
            dma((ITERS, G * N)), dma((ITERS, G * N)),
        ],
        compiler_params=pltpu.CompilerParams(collective_id=0, has_side_effects=True),
        name="pdhg",
    )(
        cost, plan,
        row_mass.reshape(groups, LANES), col_mass.reshape(chunks, LANES),
        row_dual.reshape(groups, LANES), col_dual.reshape(chunks, LANES),
    )
    return plan_out, u_out.reshape(rows), v_out.reshape(cols)


def solution(mesh):
    W, N = mesh.shape["wide"], mesh.shape["narrow"]
    G = 2 if W % 2 == 0 else 1
    in_specs = (
        P("wide", "narrow"),
        P("wide", "narrow"),
        P("wide"),
        P("narrow"),
        P("wide"),
        P("narrow"),
    )
    out_specs = (P("wide", "narrow"), P("wide"), P("narrow"))
    return jax.shard_map(
        functools.partial(shards, W, N, G),
        mesh=mesh, in_specs=in_specs, out_specs=out_specs, check_vma=False)
```

```python
import functools
import math

import jax
import jax.numpy as jnp
from jax import lax
from jax.experimental import pallas as pl
from jax.experimental.pallas import tpu as pltpu
from jax.sharding import PartitionSpec as P

ITERS = 4
LANES = 128
BLOCKS = 8
MESH = pl.DeviceIdType.MESH


def exchange(ref, k, mine, peers, send_sem, recv_sem, source=None):
    sent, waits = [], []
    for d, (to, src, device) in enumerate(peers):
        copy = pltpu.make_async_remote_copy(
            src_ref=ref.at[k, mine] if source is None else source, dst_ref=ref.at[k, mine],
            send_sem=send_sem.at[k, d], recv_sem=recv_sem.at[k, mine],
            device_id=device, device_id_type=MESH)
        copy.start()
        sent.append(copy)
        waits.append(pltpu.make_async_remote_copy(
            src_ref=ref.at[k, src], dst_ref=ref.at[k, src],
            send_sem=send_sem.at[k, d], recv_sem=recv_sem.at[k, src],
            device_id=device, device_id_type=MESH))
    return sent, waits


def arrived(waits):
    for copy in waits:
        copy.wait_recv()


def total_of(ref, k, count):
    out = ref[k, 0]
    for i in range(1, count):
        out = out + ref[k, i]
    return out


def kernel(
    W, N, step_base,
    cost_hbm, plan_hbm, rmass_hbm, cmass_hbm, u_hbm, v_hbm,
    plan_out, u_out, v_out,
    cost, plan_a, plan_b, gap, rmass, cmass, ub, ucur, V, CB, RB, RP, RH, MV, SC,
    in_sem, small_sem,
    s1_send, s1_recv, row_send, row_recv, rho_send, rho_recv,
    mv_send, mv_recv, sc_send, sc_recv,
):
    rows, cols = plan_a.shape
    chunks = cols // LANES
    groups = rows // LANES
    per_block = chunks // BLOCKS
    width = per_block * LANES
    w = lax.axis_index("wide")
    n = lax.axis_index("narrow")

    wide_peers = []
    for d in range(W - 1, 0, -1):
        to = lax.rem(w + d, W)
        wide_peers.append((to, lax.rem(w + W - d, W), (to, n)))
    narrow_peers = []
    for d in range(N - 1, 0, -1):
        to = lax.rem(n + d, N)
        narrow_peers.append((to, lax.rem(n + N - d, N), (w, to)))

    barrier = pltpu.get_barrier_semaphore()
    for _, _, device in wide_peers + narrow_peers:
        pl.semaphore_signal(barrier, inc=1, device_id=device, device_id_type=MESH)

    smalls = [
        pltpu.make_async_copy(u_hbm, ucur, small_sem.at[0]),
        pltpu.make_async_copy(v_hbm, V.at[0], small_sem.at[1]),
        pltpu.make_async_copy(rmass_hbm, rmass, small_sem.at[2]),
        pltpu.make_async_copy(cmass_hbm, cmass, small_sem.at[3]),
    ]
    for copy in smalls:
        copy.start()
    loads = []
    for b in range(BLOCKS):
        sl = (slice(None), pl.ds(b * width, width))
        pair = (
            pltpu.make_async_copy(cost_hbm.at[sl], cost.at[sl], in_sem.at[0, b]),
            pltpu.make_async_copy(plan_hbm.at[sl], plan_a.at[sl], in_sem.at[1, b]),
        )
        for copy in pair:
            copy.start()
        loads.append(pair)

    def spread(u):
        for g in range(groups):
            ub[g * LANES:(g + 1) * LANES, :] = jnp.broadcast_to(u[g:g + 1], (LANES, LANES)).T

    def to_lanes(acc):
        return jnp.concatenate(
            [
                jnp.sum(acc[g * LANES:(g + 1) * LANES].T, axis=0, keepdims=True)
                for g in range(groups)
            ],
            axis=0,
        )

    def lanes_of(c):
        return pl.ds(pl.multiple_of(c * LANES, LANES), LANES)

    for copy in smalls:
        copy.wait()
    spread(ucur[...])

    zero_rows = jnp.zeros((rows, LANES), jnp.float32)
    weight = jnp.full((1, 1), step_base, jnp.float32)
    row_old = None
    pending = []
    for k in range(ITERS):
        last = k == ITERS - 1
        old = plan_a if k % 2 == 0 else plan_b
        new = plan_out if last else (plan_b if k % 2 == 0 else plan_a)
        dual = step_base * weight
        tau = jnp.broadcast_to(step_base / weight, (1, LANES))

        if k == 0:
            def first(c, racc, old=old, new=new, tau=tau):
                lanes = lanes_of(c)
                x = old[:, lanes]
                f = jnp.maximum(
                    x - tau * (cost[:, lanes] - ub[...] - V[0, pl.ds(c, 1), :]), 0.0)
                new[:, lanes] = f
                ext = f + (f - x)
                CB[0, pl.ds(c, 1), :] = jnp.sum(ext, axis=0, keepdims=True)
                return racc + ext

            racc = zero_rows
            for b in range(BLOCKS):
                for copy in loads[b]:
                    copy.wait()
                racc = lax.fori_loop(
                    b * per_block, (b + 1) * per_block, first, racc, unroll=2)
            RB[0, w] = CB[0]
            pl.semaphore_wait(barrier, W - 1 + N - 1)
        else:
            def step(c, racc, k=k, old=old, new=new, tau=tau):
                lanes = lanes_of(c)
                f = jnp.maximum(old[:, lanes] - tau * gap[:, lanes], 0.0)
                new[:, lanes] = f
                CB[k + 1, pl.ds(c, 1), :] = jnp.sum(f, axis=0, keepdims=True)
                return racc + f

            racc = lax.fori_loop(0, chunks, step, zero_rows, unroll=4)
            RB[k, w] = 2.0 * CB[k + 1] - CB[k]

        sent, col_waits = exchange(RB, k, w, wide_peers, s1_send, s1_recv)
        pending += sent
        row_new = to_lanes(racc)
        RP[k, n] = row_new if k == 0 else 2.0 * row_new - row_old
        row_old = row_new
        sent, row_waits = exchange(RP, k, n, narrow_peers, row_send, row_recv)
        pending += sent

        if not last:
            def change(c, carry, k=k, old=old, new=new):
                lanes = lanes_of(c)
                f = new[:, lanes]
                ch = f - old[:, lanes]
                sq = jnp.sum((ch * ch).reshape(rows // 8, 8, LANES), axis=0)
                if k:
                    return (carry[0] + sq,)
                CB[1, pl.ds(c, 1), :] = jnp.sum(f, axis=0, keepdims=True)
                return carry[0] + sq, carry[1] + f

            start = (jnp.zeros((8, LANES), jnp.float32),)
            out = lax.fori_loop(
                0, chunks, change, start if k else start + (zero_rows,), unroll=2)
            MV[k, w] = jnp.sum(out[0], axis=0, keepdims=True)
            sent, mv_waits = exchange(MV, k, w, wide_peers, mv_send, mv_recv)
            pending += sent
            if k == 0:
                row_old = to_lanes(out[1])

        arrived(row_waits)
        u_old = ucur[...]
        u_new = u_old + dual * (rmass[...] - total_of(RP, k, N))
        if last:
            u_out[...] = u_new
        else:
            RH[k, w] = jnp.sum((u_new - u_old) ** 2, axis=0, keepdims=True)
            sent, rho_waits = exchange(RH, k, w, wide_peers, rho_send, rho_recv)
            pending += sent
            ucur[...] = u_new
            spread(u_new)
            arrived(mv_waits)
            SC[k, n, 1:2, :] = total_of(MV, k, W)

        arrived(col_waits)
        v_old = V[k]
        v_new = v_old + dual * (cmass[...] - total_of(RB, k, W))
        if last:
            v_out[...] = v_new
            continue
        SC[k, n, 0:1, :] = jnp.sum((v_new - v_old) ** 2, axis=0, keepdims=True)
        V[k + 1] = v_new
        sent, sc_waits = exchange(SC, k, n, narrow_peers, sc_send, sc_recv)
        pending += sent

        def reduce_cost(c, carry, k=k):
            lanes = lanes_of(c)
            gap[:, lanes] = cost[:, lanes] - ub[...] - V[k + 1, pl.ds(c, 1), :]
            return carry

        lax.fori_loop(0, chunks, reduce_cost, 0, unroll=2)
        arrived(rho_waits)
        rho = total_of(RH, k, W)
        arrived(sc_waits)
        both = total_of(SC, k, N)
        dual_moved = jnp.sum(rho + both[0:1], axis=1, keepdims=True)
        moved = jnp.sum(both[1:2], axis=1, keepdims=True)
        weight = jnp.sqrt(weight * jnp.sqrt((dual_moved + 1.0) / (moved + 1.0)))
    for copy in pending:
        copy.wait_send()


def shards(W, N, cost, plan, row_mass, col_mass, row_dual, col_dual):
    rows, cols = plan.shape
    step_base = 0.9 / math.sqrt(rows * W + cols * N)
    chunks = cols // LANES
    groups = rows // LANES
    f32 = jnp.float32
    dma = pltpu.SemaphoreType.DMA
    vmem = pl.BlockSpec(memory_space=pltpu.VMEM)
    hbm = pl.BlockSpec(memory_space=pl.ANY)
    plan_out, u_out, v_out = pl.pallas_call(
        functools.partial(kernel, W, N, step_base),
        out_shape=(
            pltpu.VMEM((rows, cols), f32),
            pltpu.VMEM((groups, LANES), f32),
            pltpu.VMEM((chunks, LANES), f32),
        ),
        in_specs=[hbm] * 6,
        out_specs=(vmem, vmem, vmem),
        scratch_shapes=[
            pltpu.VMEM((rows, cols), f32),
            pltpu.VMEM((rows, cols), f32),
            pltpu.VMEM((rows, cols), f32),
            pltpu.VMEM((rows, cols), f32),
            pltpu.VMEM((groups, LANES), f32),
            pltpu.VMEM((chunks, LANES), f32),
            pltpu.VMEM((rows, LANES), f32),
            pltpu.VMEM((groups, LANES), f32),
            pltpu.VMEM((ITERS, chunks, LANES), f32),
            pltpu.VMEM((ITERS + 1, chunks, LANES), f32),
            pltpu.VMEM((ITERS, W, chunks, LANES), f32),
            pltpu.VMEM((ITERS, N, groups, LANES), f32),
            pltpu.VMEM((ITERS, W, 1, LANES), f32),
            pltpu.VMEM((ITERS, W, 1, LANES), f32),
            pltpu.VMEM((ITERS, N, 2, LANES), f32),
            dma((2, BLOCKS)), dma((4,)),
            dma((ITERS, W)), dma((ITERS, W)),
            dma((ITERS, N)), dma((ITERS, N)),
            dma((ITERS, W)), dma((ITERS, W)),
            dma((ITERS, W)), dma((ITERS, W)),
            dma((ITERS, N)), dma((ITERS, N)),
        ],
        compiler_params=pltpu.CompilerParams(collective_id=0, has_side_effects=True),
        name="pdhg",
    )(
        cost, plan,
        row_mass.reshape(groups, LANES), col_mass.reshape(chunks, LANES),
        row_dual.reshape(groups, LANES), col_dual.reshape(chunks, LANES),
    )
    return plan_out, u_out.reshape(rows), v_out.reshape(cols)


def solution(mesh):
    in_specs = (
        P("wide", "narrow"),
        P("wide", "narrow"),
        P("wide"),
        P("narrow"),
        P("wide"),
        P("narrow"),
    )
    out_specs = (P("wide", "narrow"), P("wide"), P("narrow"))
    return jax.shard_map(
        functools.partial(shards, mesh.shape["wide"], mesh.shape["narrow"]),
        mesh=mesh, in_specs=in_specs, out_specs=out_specs, check_vma=False)
```

```python
import functools
import math

import jax
import jax.numpy as jnp
from jax import lax
from jax.experimental import pallas as pl
from jax.experimental.pallas import tpu as pltpu
from jax.sharding import PartitionSpec as P

ITERS = 4
LANES = 128
BLOCKS = 8
MESH = pl.DeviceIdType.MESH


def exchange(ref, k, mine, peers, send_sem, recv_sem, source=None):
    sent, waits = [], []
    for d, (to, src, device) in enumerate(peers):
        copy = pltpu.make_async_remote_copy(
            src_ref=ref.at[k, mine] if source is None else source, dst_ref=ref.at[k, mine],
            send_sem=send_sem.at[k, d], recv_sem=recv_sem.at[k, mine],
            device_id=device, device_id_type=MESH)
        copy.start()
        sent.append(copy)
        waits.append(pltpu.make_async_remote_copy(
            src_ref=ref.at[k, src], dst_ref=ref.at[k, src],
            send_sem=send_sem.at[k, d], recv_sem=recv_sem.at[k, src],
            device_id=device, device_id_type=MESH))
    return sent, waits


def arrived(waits):
    for copy in waits:
        copy.wait_recv()


def total_of(ref, k, count):
    out = ref[k, 0]
    for i in range(1, count):
        out = out + ref[k, i]
    return out


def kernel(
    W, N, step_base,
    cost_hbm, plan_hbm, rmass_hbm, cmass_hbm, u_hbm, v_hbm,
    plan_out, u_out, v_out,
    cost, plan_a, plan_b, gap, rmass, cmass, ub, ucur, V, CB, fold, RB, RP, RH, MV, SC,
    in_sem, small_sem,
    s1_send, s1_recv, row_send, row_recv, rho_send, rho_recv,
    mv_send, mv_recv, sc_send, sc_recv,
):
    rows, cols = plan_a.shape
    chunks = cols // LANES
    groups = rows // LANES
    per_block = chunks // BLOCKS
    width = per_block * LANES
    w = lax.axis_index("wide")
    n = lax.axis_index("narrow")

    wide_peers = []
    for d in range(W - 1, 0, -1):
        to = lax.rem(w + d, W)
        wide_peers.append((to, lax.rem(w + W - d, W), (to, n)))
    narrow_peers = []
    for d in range(N - 1, 0, -1):
        to = lax.rem(n + d, N)
        narrow_peers.append((to, lax.rem(n + N - d, N), (w, to)))

    barrier = pltpu.get_barrier_semaphore()
    for _, _, device in wide_peers + narrow_peers:
        pl.semaphore_signal(barrier, inc=1, device_id=device, device_id_type=MESH)

    smalls = [
        pltpu.make_async_copy(u_hbm, ucur, small_sem.at[0]),
        pltpu.make_async_copy(v_hbm, V.at[0], small_sem.at[1]),
        pltpu.make_async_copy(rmass_hbm, rmass, small_sem.at[2]),
        pltpu.make_async_copy(cmass_hbm, cmass, small_sem.at[3]),
    ]
    for copy in smalls:
        copy.start()
    loads = []
    for b in range(BLOCKS):
        sl = (slice(None), pl.ds(b * width, width))
        pair = (
            pltpu.make_async_copy(cost_hbm.at[sl], cost.at[sl], in_sem.at[0, b]),
            pltpu.make_async_copy(plan_hbm.at[sl], plan_a.at[sl], in_sem.at[1, b]),
        )
        for copy in pair:
            copy.start()
        loads.append(pair)

    def spread(u):
        for g in range(groups):
            ub[g * LANES:(g + 1) * LANES, :] = jnp.broadcast_to(u[g:g + 1], (LANES, LANES)).T

    def to_lanes(acc):
        return jnp.concatenate(
            [
                jnp.sum(acc[g * LANES:(g + 1) * LANES].T, axis=0, keepdims=True)
                for g in range(groups)
            ],
            axis=0,
        )

    def by_sublane(x):
        return jnp.sum(x.reshape(rows // 8, 8, LANES), axis=0)

    def keep_columns(c, x):
        fold[pl.ds(pl.multiple_of(c * 8, 8), 8), :] = by_sublane(x)

    def columns():
        out = fold[pl.ds(0, chunks, stride=8), :]
        for i in range(1, 8):
            out = out + fold[pl.ds(i, chunks, stride=8), :]
        return out

    def lanes_of(c):
        return pl.ds(pl.multiple_of(c * LANES, LANES), LANES)

    for copy in smalls:
        copy.wait()
    spread(ucur[...])

    zero_rows = jnp.zeros((rows, LANES), jnp.float32)
    weight = jnp.full((1, 1), step_base, jnp.float32)
    tau = jnp.ones((1, LANES), jnp.float32)
    row_old = None
    pending = []
    for k in range(ITERS):
        last = k == ITERS - 1
        old = plan_a if k % 2 == 0 else plan_b
        new = plan_out if last else (plan_b if k % 2 == 0 else plan_a)
        dual = step_base * weight

        if k == 0:
            def first(c, racc, old=old, new=new, tau=tau):
                lanes = lanes_of(c)
                x = old[:, lanes]
                f = jnp.maximum(
                    x - tau * (cost[:, lanes] - ub[...] - V[0, pl.ds(c, 1), :]), 0.0)
                new[:, lanes] = f
                ext = f + (f - x)
                keep_columns(c, ext)
                return racc + ext

            racc = zero_rows
            for b in range(BLOCKS):
                for copy in loads[b]:
                    copy.wait()
                racc = lax.fori_loop(
                    b * per_block, (b + 1) * per_block, first, racc, unroll=2)
            RB[0, w] = columns()
            pl.semaphore_wait(barrier, W - 1 + N - 1)
        else:
            def step(c, racc, k=k, old=old, new=new, tau=tau):
                lanes = lanes_of(c)
                f = jnp.maximum(old[:, lanes] - tau * gap[:, lanes], 0.0)
                new[:, lanes] = f
                keep_columns(c, f)
                return racc + f

            racc = lax.fori_loop(0, chunks, step, zero_rows, unroll=32)
            fresh_cols = columns()
            RB[k, w] = 2.0 * fresh_cols - CB[...]
            CB[...] = fresh_cols

        sent, col_waits = exchange(RB, k, w, wide_peers, s1_send, s1_recv)
        pending += sent
        row_new = to_lanes(racc)
        RP[k, n] = row_new if k == 0 else 2.0 * row_new - row_old
        row_old = row_new
        sent, row_waits = exchange(RP, k, n, narrow_peers, row_send, row_recv)
        pending += sent

        if not last:
            def change(c, carry, k=k, old=old, new=new):
                lanes = lanes_of(c)
                f = new[:, lanes]
                ch = f - old[:, lanes]
                sq = by_sublane(ch * ch)
                if k:
                    return (carry[0] + sq,)
                keep_columns(c, f)
                return carry[0] + sq, carry[1] + f

            start = (jnp.zeros((8, LANES), jnp.float32),)
            out = lax.fori_loop(
                0, chunks, change, start if k else start + (zero_rows,), unroll=2)
            MV[k, n] = jnp.sum(out[0], axis=0, keepdims=True)
            sent, mv_waits = exchange(MV, k, n, narrow_peers, mv_send, mv_recv)
            pending += sent
            if k == 0:
                row_old = to_lanes(out[1])
                CB[...] = columns()

        arrived(row_waits)
        u_old = ucur[...]
        u_new = u_old + dual * (rmass[...] - total_of(RP, k, N))
        if last:
            u_out[...] = u_new
        else:
            RH[k, w, 0:1, :] = jnp.sum((u_new - u_old) ** 2, axis=0, keepdims=True)
            arrived(mv_waits)
            RH[k, w, 1:2, :] = total_of(MV, k, N)
            sent, rho_waits = exchange(RH, k, w, wide_peers, rho_send, rho_recv)
            pending += sent
            ucur[...] = u_new
            spread(u_new)

        arrived(col_waits)
        v_old = V[k]
        v_new = v_old + dual * (cmass[...] - total_of(RB, k, W))
        if last:
            v_out[...] = v_new
            continue
        SC[k, n] = jnp.sum((v_new - v_old) ** 2, axis=0, keepdims=True)
        V[k + 1] = v_new
        sent, sc_waits = exchange(SC, k, n, narrow_peers, sc_send, sc_recv)
        pending += sent

        def reduce_cost(c, carry, k=k):
            lanes = lanes_of(c)
            gap[:, lanes] = cost[:, lanes] - ub[...] - V[k + 1, pl.ds(c, 1), :]
            return carry

        lax.fori_loop(0, chunks, reduce_cost, 0, unroll=2)
        arrived(rho_waits)
        known = jnp.sum(total_of(RH, k, W), axis=1, keepdims=True)
        known_dual = known[0:1] + 1.0
        per_moved = 1.0 / (known[1:2] + 1.0)
        arrived(sc_waits)
        col_square = jnp.sum(total_of(SC, k, N), axis=1, keepdims=True)
        square = weight * jnp.sqrt((known_dual + col_square) * per_moved)
        tau = jnp.broadcast_to(step_base * lax.rsqrt(square), (1, LANES))
        weight = jnp.sqrt(square)
    for copy in pending:
        copy.wait_send()


def store(plan, u, v, plan_hbm, u_hbm, v_hbm, sem):
    height = plan.shape[0] // BLOCKS
    copies = [
        pltpu.make_async_copy(u, u_hbm, sem.at[BLOCKS]),
        pltpu.make_async_copy(v, v_hbm, sem.at[BLOCKS + 1]),
    ]
    for b in range(BLOCKS):
        sl = pl.ds(b * height, height)
        copies.append(pltpu.make_async_copy(plan.at[sl], plan_hbm.at[sl], sem.at[b]))
    for copy in copies:
        copy.start()
    for copy in copies:
        copy.wait()


def shards(W, N, cost, plan, row_mass, col_mass, row_dual, col_dual):
    rows, cols = plan.shape
    step_base = 0.9 / math.sqrt(rows * W + cols * N)
    chunks = cols // LANES
    groups = rows // LANES
    f32 = jnp.float32
    dma = pltpu.SemaphoreType.DMA
    vmem = pl.BlockSpec(memory_space=pltpu.VMEM)
    hbm = pl.BlockSpec(memory_space=pl.ANY)
    plan_out, u_out, v_out = pl.pallas_call(
        functools.partial(kernel, W, N, step_base),
        out_shape=(
            pltpu.VMEM((rows, cols), f32),
            pltpu.VMEM((groups, LANES), f32),
            pltpu.VMEM((chunks, LANES), f32),
        ),
        in_specs=[hbm] * 6,
        out_specs=(vmem, vmem, vmem),
        scratch_shapes=[
            pltpu.VMEM((rows, cols), f32),
            pltpu.VMEM((rows, cols), f32),
            pltpu.VMEM((rows, cols), f32),
            pltpu.VMEM((rows, cols), f32),
            pltpu.VMEM((groups, LANES), f32),
            pltpu.VMEM((chunks, LANES), f32),
            pltpu.VMEM((rows, LANES), f32),
            pltpu.VMEM((groups, LANES), f32),
            pltpu.VMEM((ITERS, chunks, LANES), f32),
            pltpu.VMEM((chunks, LANES), f32),
            pltpu.VMEM((chunks * 8, LANES), f32),
            pltpu.VMEM((ITERS, W, chunks, LANES), f32),
            pltpu.VMEM((ITERS, N, groups, LANES), f32),
            pltpu.VMEM((ITERS, W, 2, LANES), f32),
            pltpu.VMEM((ITERS, N, 1, LANES), f32),
            pltpu.VMEM((ITERS, N, 1, LANES), f32),
            dma((2, BLOCKS)), dma((4,)),
            dma((ITERS, W)), dma((ITERS, W)),
            dma((ITERS, N)), dma((ITERS, N)),
            dma((ITERS, W)), dma((ITERS, W)),
            dma((ITERS, N)), dma((ITERS, N)),
            dma((ITERS, N)), dma((ITERS, N)),
        ],
        compiler_params=pltpu.CompilerParams(collective_id=0, has_side_effects=True),
        name="pdhg",
    )(
        cost, plan,
        row_mass.reshape(groups, LANES), col_mass.reshape(chunks, LANES),
        row_dual.reshape(groups, LANES), col_dual.reshape(chunks, LANES),
    )
    keep = functools.partial(pltpu.with_memory_space_constraint, memory_space=pltpu.VMEM)
    plan_out, u_out, v_out = pl.pallas_call(
        store,
        out_shape=(
            jax.ShapeDtypeStruct((rows, cols), f32),
            jax.ShapeDtypeStruct((groups, LANES), f32),
            jax.ShapeDtypeStruct((chunks, LANES), f32),
        ),
        in_specs=[vmem, vmem, vmem],
        out_specs=(hbm, hbm, hbm),
        scratch_shapes=[dma((BLOCKS + 2,))],
        name="store",
    )(keep(plan_out), keep(u_out), keep(v_out))
    return plan_out, u_out.reshape(rows), v_out.reshape(cols)


def solution(mesh):
    in_specs = (
        P("wide", "narrow"),
        P("wide", "narrow"),
        P("wide"),
        P("narrow"),
        P("wide"),
        P("narrow"),
    )
    out_specs = (P("wide", "narrow"), P("wide"), P("narrow"))
    return jax.shard_map(
        functools.partial(shards, mesh.shape["wide"], mesh.shape["narrow"]),
        mesh=mesh, in_specs=in_specs, out_specs=out_specs, check_vma=False)
```

```python
import functools
import math

import jax
import jax.numpy as jnp
from jax import lax
from jax.experimental import pallas as pl
from jax.experimental.pallas import tpu as pltpu
from jax.sharding import PartitionSpec as P

ITERS = 4
LANES = 128
BLOCKS = 8
MESH = pl.DeviceIdType.MESH


def exchange(ref, k, mine, peers, send_sem, recv_sem, source=None):
    sent, waits = [], []
    for d, (to, src, device) in enumerate(peers):
        copy = pltpu.make_async_remote_copy(
            src_ref=ref.at[k, mine] if source is None else source, dst_ref=ref.at[k, mine],
            send_sem=send_sem.at[k, d], recv_sem=recv_sem.at[k, mine],
            device_id=device, device_id_type=MESH)
        copy.start()
        sent.append(copy)
        waits.append(pltpu.make_async_remote_copy(
            src_ref=ref.at[k, src], dst_ref=ref.at[k, src],
            send_sem=send_sem.at[k, d], recv_sem=recv_sem.at[k, src],
            device_id=device, device_id_type=MESH))
    return sent, waits


def arrived(waits):
    for copy in waits:
        copy.wait_recv()


def total_of(ref, k, count):
    out = ref[k, 0]
    for i in range(1, count):
        out = out + ref[k, i]
    return out


def kernel(
    W, N, step_base,
    cost_hbm, plan_hbm, rmass_hbm, cmass_hbm, u_hbm, v_hbm,
    plan_out, u_out, v_out,
    cost, plan_a, plan_b, gap, rmass, cmass, ub, ucur, V, CB, fold, RB, RP, RH, MV, SC,
    in_sem, small_sem,
    s1_send, s1_recv, row_send, row_recv, rho_send, rho_recv,
    mv_send, mv_recv, sc_send, sc_recv,
):
    rows, cols = plan_a.shape
    chunks = cols // LANES
    groups = rows // LANES
    per_block = chunks // BLOCKS
    width = per_block * LANES
    w = lax.axis_index("wide")
    n = lax.axis_index("narrow")

    wide_peers = []
    for d in sorted(range(1, W), key=lambda d: (d % 2 == 0, d)):
        to = lax.rem(w + d, W)
        wide_peers.append((to, lax.rem(w + W - d, W), (to, n)))
    narrow_peers = []
    for d in range(N - 1, 0, -1):
        to = lax.rem(n + d, N)
        narrow_peers.append((to, lax.rem(n + N - d, N), (w, to)))

    barrier = pltpu.get_barrier_semaphore()
    for _, _, device in wide_peers + narrow_peers:
        pl.semaphore_signal(barrier, inc=1, device_id=device, device_id_type=MESH)

    smalls = [
        pltpu.make_async_copy(u_hbm, ucur, small_sem.at[0]),
        pltpu.make_async_copy(v_hbm, V.at[0], small_sem.at[1]),
        pltpu.make_async_copy(rmass_hbm, rmass, small_sem.at[2]),
        pltpu.make_async_copy(cmass_hbm, cmass, small_sem.at[3]),
    ]
    for copy in smalls:
        copy.start()
    loads = []
    for b in range(BLOCKS):
        sl = (slice(None), pl.ds(b * width, width))
        pair = (
            pltpu.make_async_copy(cost_hbm.at[sl], cost.at[sl], in_sem.at[0, b]),
            pltpu.make_async_copy(plan_hbm.at[sl], plan_a.at[sl], in_sem.at[1, b]),
        )
        for copy in pair:
            copy.start()
        loads.append(pair)

    def spread(u):
        for g in range(groups):
            ub[g * LANES:(g + 1) * LANES, :] = jnp.broadcast_to(u[g:g + 1], (LANES, LANES)).T

    def to_lanes(acc):
        return jnp.concatenate(
            [
                jnp.sum(acc[g * LANES:(g + 1) * LANES].T, axis=0, keepdims=True)
                for g in range(groups)
            ],
            axis=0,
        )

    def by_sublane(x):
        return jnp.sum(x.reshape(rows // 8, 8, LANES), axis=0)

    def keep_columns(c, x):
        fold[pl.ds(pl.multiple_of(c * 8, 8), 8), :] = by_sublane(x)

    def columns():
        out = fold[pl.ds(0, chunks, stride=8), :]
        for i in range(1, 8):
            out = out + fold[pl.ds(i, chunks, stride=8), :]
        return out

    def lanes_of(c):
        return pl.ds(pl.multiple_of(c * LANES, LANES), LANES)

    for copy in smalls:
        copy.wait()
    spread(ucur[...])

    zero_rows = jnp.zeros((rows, LANES), jnp.float32)
    weight = jnp.full((1, 1), step_base, jnp.float32)
    tau = jnp.ones((1, LANES), jnp.float32)
    row_old = None
    pending = []
    for k in range(ITERS):
        last = k == ITERS - 1
        old = plan_a if k % 2 == 0 else plan_b
        new = plan_out if last else (plan_b if k % 2 == 0 else plan_a)
        dual = step_base * weight

        if k == 0:
            def first(c, racc, old=old, new=new, tau=tau):
                lanes = lanes_of(c)
                x = old[:, lanes]
                f = jnp.maximum(
                    x - tau * (cost[:, lanes] - ub[...] - V[0, pl.ds(c, 1), :]), 0.0)
                new[:, lanes] = f
                ext = f + (f - x)
                keep_columns(c, ext)
                return racc + ext

            racc = zero_rows
            for b in range(BLOCKS):
                for copy in loads[b]:
                    copy.wait()
                racc = lax.fori_loop(
                    b * per_block, (b + 1) * per_block, first, racc, unroll=2)
            RB[0, w] = columns()
            pl.semaphore_wait(barrier, W - 1 + N - 1)
        else:
            def step(c, racc, k=k, old=old, new=new, tau=tau):
                lanes = lanes_of(c)
                f = jnp.maximum(old[:, lanes] - tau * gap[:, lanes], 0.0)
                new[:, lanes] = f
                keep_columns(c, f)
                return racc + f

            racc = lax.fori_loop(0, chunks, step, zero_rows, unroll=32)
            fresh_cols = columns()
            RB[k, w] = 2.0 * fresh_cols - CB[...]
            CB[...] = fresh_cols

        sent, col_waits = exchange(RB, k, w, wide_peers, s1_send, s1_recv)
        pending += sent
        row_new = to_lanes(racc)
        RP[k, n] = row_new if k == 0 else 2.0 * row_new - row_old
        row_old = row_new
        sent, row_waits = exchange(RP, k, n, narrow_peers, row_send, row_recv)
        pending += sent

        if not last:
            def change(c, carry, k=k, old=old, new=new):
                lanes = lanes_of(c)
                f = new[:, lanes]
                ch = f - old[:, lanes]
                sq = by_sublane(ch * ch)
                if k:
                    return (carry[0] + sq,)
                keep_columns(c, f)
                return carry[0] + sq, carry[1] + f

            start = (jnp.zeros((8, LANES), jnp.float32),)
            out = lax.fori_loop(
                0, chunks, change, start if k else start + (zero_rows,), unroll=8)
            MV[k, n] = jnp.sum(out[0], axis=0, keepdims=True)
            sent, mv_waits = exchange(MV, k, n, narrow_peers, mv_send, mv_recv)
            pending += sent
            if k == 0:
                row_old = to_lanes(out[1])
                CB[...] = columns()

        arrived(row_waits)
        u_old = ucur[...]
        u_new = u_old + dual * (rmass[...] - total_of(RP, k, N))
        if last:
            u_out[...] = u_new
        else:
            RH[k, w, 0:1, :] = jnp.sum((u_new - u_old) ** 2, axis=0, keepdims=True)
            arrived(mv_waits)
            RH[k, w, 1:2, :] = total_of(MV, k, N)
            sent, rho_waits = exchange(RH, k, w, wide_peers, rho_send, rho_recv)
            pending += sent
            ucur[...] = u_new
            spread(u_new)

        arrived(col_waits)
        v_old = V[k]
        v_new = v_old + dual * (cmass[...] - total_of(RB, k, W))
        if last:
            v_out[...] = v_new
            continue
        SC[k, n] = jnp.sum((v_new - v_old) ** 2, axis=0, keepdims=True)
        V[k + 1] = v_new
        sent, sc_waits = exchange(SC, k, n, narrow_peers, sc_send, sc_recv)
        pending += sent

        def reduce_cost(c, carry, k=k):
            lanes = lanes_of(c)
            gap[:, lanes] = cost[:, lanes] - ub[...] - V[k + 1, pl.ds(c, 1), :]
            return carry

        lax.fori_loop(0, chunks, reduce_cost, 0, unroll=8)
        arrived(rho_waits)
        known = jnp.sum(total_of(RH, k, W), axis=1, keepdims=True)
        known_dual = known[0:1] + 1.0
        per_moved = 1.0 / (known[1:2] + 1.0)
        arrived(sc_waits)
        col_square = jnp.sum(total_of(SC, k, N), axis=1, keepdims=True)
        square = weight * jnp.sqrt((known_dual + col_square) * per_moved)
        tau = jnp.broadcast_to(step_base * lax.rsqrt(square), (1, LANES))
        weight = jnp.sqrt(square)
    for copy in pending:
        copy.wait_send()


def store(plan, u, v, plan_hbm, u_hbm, v_hbm, sem):
    height = plan.shape[0] // BLOCKS
    copies = [
        pltpu.make_async_copy(u, u_hbm, sem.at[BLOCKS]),
        pltpu.make_async_copy(v, v_hbm, sem.at[BLOCKS + 1]),
    ]
    for b in range(BLOCKS):
        sl = pl.ds(b * height, height)
        copies.append(pltpu.make_async_copy(plan.at[sl], plan_hbm.at[sl], sem.at[b]))
    for copy in copies:
        copy.start()
    for copy in copies:
        copy.wait()


def shards(W, N, cost, plan, row_mass, col_mass, row_dual, col_dual):
    rows, cols = plan.shape
    step_base = 0.9 / math.sqrt(rows * W + cols * N)
    chunks = cols // LANES
    groups = rows // LANES
    f32 = jnp.float32
    dma = pltpu.SemaphoreType.DMA
    vmem = pl.BlockSpec(memory_space=pltpu.VMEM)
    hbm = pl.BlockSpec(memory_space=pl.ANY)
    plan_out, u_out, v_out = pl.pallas_call(
        functools.partial(kernel, W, N, step_base),
        out_shape=(
            pltpu.VMEM((rows, cols), f32),
            pltpu.VMEM((groups, LANES), f32),
            pltpu.VMEM((chunks, LANES), f32),
        ),
        in_specs=[hbm] * 6,
        out_specs=(vmem, vmem, vmem),
        scratch_shapes=[
            pltpu.VMEM((rows, cols), f32),
            pltpu.VMEM((rows, cols), f32),
            pltpu.VMEM((rows, cols), f32),
            pltpu.VMEM((rows, cols), f32),
            pltpu.VMEM((groups, LANES), f32),
            pltpu.VMEM((chunks, LANES), f32),
            pltpu.VMEM((rows, LANES), f32),
            pltpu.VMEM((groups, LANES), f32),
            pltpu.VMEM((ITERS, chunks, LANES), f32),
            pltpu.VMEM((chunks, LANES), f32),
            pltpu.VMEM((chunks * 8, LANES), f32),
            pltpu.VMEM((ITERS, W, chunks, LANES), f32),
            pltpu.VMEM((ITERS, N, groups, LANES), f32),
            pltpu.VMEM((ITERS, W, 2, LANES), f32),
            pltpu.VMEM((ITERS, N, 1, LANES), f32),
            pltpu.VMEM((ITERS, N, 1, LANES), f32),
            dma((2, BLOCKS)), dma((4,)),
            dma((ITERS, W)), dma((ITERS, W)),
            dma((ITERS, N)), dma((ITERS, N)),
            dma((ITERS, W)), dma((ITERS, W)),
            dma((ITERS, N)), dma((ITERS, N)),
            dma((ITERS, N)), dma((ITERS, N)),
        ],
        compiler_params=pltpu.CompilerParams(collective_id=0, has_side_effects=True),
        name="pdhg",
    )(
        cost, plan,
        row_mass.reshape(groups, LANES), col_mass.reshape(chunks, LANES),
        row_dual.reshape(groups, LANES), col_dual.reshape(chunks, LANES),
    )
    keep = functools.partial(pltpu.with_memory_space_constraint, memory_space=pltpu.VMEM)
    plan_out, u_out, v_out = pl.pallas_call(
        store,
        out_shape=(
            jax.ShapeDtypeStruct((rows, cols), f32),
            jax.ShapeDtypeStruct((groups, LANES), f32),
            jax.ShapeDtypeStruct((chunks, LANES), f32),
        ),
        in_specs=[vmem, vmem, vmem],
        out_specs=(hbm, hbm, hbm),
        scratch_shapes=[dma((BLOCKS + 2,))],
        name="store",
    )(keep(plan_out), keep(u_out), keep(v_out))
    return plan_out, u_out.reshape(rows), v_out.reshape(cols)


def solution(mesh):
    in_specs = (
        P("wide", "narrow"),
        P("wide", "narrow"),
        P("wide"),
        P("narrow"),
        P("wide"),
        P("narrow"),
    )
    out_specs = (P("wide", "narrow"), P("wide"), P("narrow"))
    return jax.shard_map(
        functools.partial(shards, mesh.shape["wide"], mesh.shape["narrow"]),
        mesh=mesh, in_specs=in_specs, out_specs=out_specs, check_vma=False)
```
